32 devices in a mesh: dp: 4 (over z), mp: 8 (over y, x, core).
Axes of the slice: x: 2, y: 2, z: 4, core: 2. Of those that a mesh axis runs over, the one named last changes fastest.
Arguments:
- crop_hidden: bfloat16 [8, 768, 8192], P(None, 'dp', 'mp'), may hold values from -15 to 15
- projector_weight: bfloat16 [8192, 8192], P('mp'), may hold values from -0.21213203 to 0.21213203
- pairing: int32 [8, 768], P(None, 'dp'), may hold values from 0 to 191, as said below
Outputs:
- embeddings: float32 [8192, 8, 768], P('mp', 'dp')
- loss_terms: float32 [4], replicated
The draws below stay inside these ranges and needn't reach their ends.
Inputs may be any that keep to these rules, and one draw needn't show every extreme that they name: Each aligned block of 192 entries of a row of pairing is a permutation of 0 to 191.
All inputs are finite; a program needn't handle non-finite values.
Results may differ from the reference program's by a relative error of at most 0.0003.
Values may be sent and summed in bfloat16 or wider, within the bound.
A program may use at most 128 MiB of HBM per device.

```python
import math
import jax
import jax.numpy as jnp
from jax import lax

P_SIZE = 8192
CROPS = 8
B_DEV = 192
BATCH = 768


def latent_field(latent_key, basis_key, exponent):
    latent_width = 512
    ranks = jnp.arange(1, latent_width + 1, dtype=jnp.float32)
    spectrum = ranks ** (-exponent)
    spectrum = spectrum / jnp.sum(spectrum)
    latent = jax.random.normal(latent_key, (CROPS * BATCH, latent_width), jnp.float32) * jnp.sqrt(spectrum)[None, :]
    basis = jnp.clip(jax.random.normal(basis_key, (latent_width, P_SIZE), jnp.float32), -6.0, 6.0)
    mixed = jnp.dot(latent, basis, precision=jax.lax.Precision.HIGHEST)
    return mixed.reshape(CROPS, BATCH, P_SIZE)


def draw_crop_hidden(key, part):
    noise_key = jax.random.fold_in(key, 0)
    scale_key = jax.random.fold_in(key, 1)
    latent_key = jax.random.fold_in(key, 3)
    basis_key = jax.random.fold_in(key, 4)
    row_scale = jnp.exp(jax.random.uniform(scale_key, (CROPS, BATCH, 1), jnp.float32, math.log(0.4), math.log(2.5)))
    noise = jnp.clip(jax.random.normal(noise_key, (CROPS, BATCH, P_SIZE), jnp.float32), -6.0, 6.0)
    correlated = latent_field(latent_key, basis_key, 0.7)
    values = 0.837 * correlated + 0.548 * noise
    values = jnp.clip(values, -6.0, 6.0)
    return (values * row_scale).astype(jnp.bfloat16)


def draw_projector_weight(key, part):
    noise_key, column_key = jax.random.split(key, 2)
    column_scale = jnp.exp(jax.random.uniform(column_key, (1, P_SIZE), jnp.float32, math.log(0.1), math.log(1.6)))
    values = jnp.clip(jax.random.normal(noise_key, (P_SIZE, P_SIZE), jnp.float32), -6.0, 6.0) * column_scale / P_SIZE ** 0.5
    return values.astype(jnp.bfloat16)


def draw_pairing(key, part):
    block_keys = jax.random.split(key, CROPS * (BATCH // B_DEV))
    shuffled = jax.vmap(lambda one_key: jax.random.permutation(one_key, B_DEV))(block_keys)
    return shuffled.reshape(CROPS, BATCH).astype(jnp.int32)


def setup_inputs(seed: int = 0) -> dict:
    splits = jax.random.split(jax.random.key(seed), 4)
    crop_hidden = draw_crop_hidden(jax.random.fold_in(splits[3], 71), 0)
    projector_weight = draw_projector_weight(jax.random.fold_in(splits[3], 71), 0)
    pairing = draw_pairing(jax.random.fold_in(splits[3], 71), 0)
    return dict(crop_hidden=crop_hidden, projector_weight=projector_weight, pairing=pairing)


def reference(crop_hidden, projector_weight, pairing):
    flat_rows = crop_hidden.reshape(CROPS * BATCH, P_SIZE)
    embedded = jnp.dot(flat_rows, projector_weight, preferred_element_type=jnp.float32)
    embeddings = jnp.transpose(embedded.reshape(CROPS, BATCH, P_SIZE), (2, 0, 1))
    block_start = jnp.arange(BATCH, dtype=jnp.int32) // B_DEV * B_DEV
    aligned_list = []
    for crop_index in range(CROPS):
        image_index = (block_start + pairing[crop_index]).astype(jnp.int32)
        image_order = jnp.argsort(image_index).astype(jnp.int32)
        aligned_list.append(jnp.take(embeddings[:, crop_index, :], image_order, axis=1))
    aligned = jnp.stack(aligned_list, axis=1)
    invariance = 0.0
    for anchor in range(2):
        differ = aligned - aligned[:, anchor:anchor + 1, :]
        invariance = invariance + jnp.sum(differ * differ)
    invariance_loss = invariance / (2 * (CROPS - 1) * BATCH * P_SIZE)
    hinge_total = 0.0
    off_total = 0.0
    for crop_index in range(CROPS):
        values = embeddings[:, crop_index, :]
        centered = values - lax.optimization_barrier(jnp.mean(values, axis=1, keepdims=True))
        variance = lax.optimization_barrier(jnp.sum(centered * centered, axis=1)) / (BATCH - 1)
        hinge_total = hinge_total + jnp.sum(jax.nn.relu(1.0 - jnp.sqrt(variance + 0.0001)))
        gram_block = jnp.dot(centered.T, centered, precision=lax.Precision.HIGHEST)
        off_total = off_total + jnp.sum(gram_block * gram_block) / ((BATCH - 1) * (BATCH - 1)) - jnp.sum(variance * variance)
    variance_loss = hinge_total / (CROPS * P_SIZE)
    covariance_loss = off_total / (CROPS * P_SIZE)
    total_loss = 25.0 * invariance_loss + 25.0 * variance_loss + covariance_loss
    loss_terms = jnp.stack([invariance_loss, variance_loss, covariance_loss, total_loss]).astype(jnp.float32)
    return (embeddings, loss_terms)
```

```python
import jax
import jax.numpy as jnp
from jax import lax
from jax.sharding import PartitionSpec as P

epsilon = 0.0001
segments = 2


def coded(values):
    top = jnp.maximum(jnp.max(jnp.abs(values), axis=-1, keepdims=True), 1e-30)
    codes = jnp.round(values * (32767.0 / top)).astype(jnp.int16)
    return codes, top * (1.0 / 32767.0)


def moved(values, axis, pairs):
    codes, step = coded(values)
    codes = lax.ppermute(codes, axis, pairs)
    step = lax.ppermute(step, axis, pairs)
    return codes.astype(jnp.float32) * step


def reduced_segments(hidden, weight, mp_size):
    me = lax.axis_index("mp")
    block = weight.shape[1] // mp_size
    size = block // segments
    partner = [(i, i ^ 1) for i in range(mp_size)]
    other_hidden = lax.ppermute(hidden, "mp", partner)
    high_bits = [1 << b for b in range(1, mp_size.bit_length() - 1)]

    def columns(relative, segment, parity):
        start = (me ^ relative ^ parity) * block + segment * size
        return lax.dynamic_slice_in_dim(weight, start, size, axis=1)

    def product(relative, segment, earlier):
        mine = columns(relative, segment, 0)
        theirs = lax.ppermute(columns(relative, segment, 1), "mp", partner)
        if earlier is not None:
            mine, theirs, earlier = lax.optimization_barrier((mine, theirs, earlier))
        terms = [
            lax.dot_general(
                w, h, (((0,), (2,)), ((), ())), preferred_element_type=jnp.float32
            )
            for w, h in ((mine, hidden), (theirs, other_hidden))
        ]
        return (terms[0] + terms[1]).transpose(1, 0, 2), earlier

    orders = [high_bits if s % 2 == 0 else high_bits[::-1] for s in range(segments)]
    offsets = []
    for order in orders:
        listed = [0]
        for bit in order[::-1]:
            listed = listed + [o | bit for o in listed]
        offsets.append(listed[::-1])
    held = [{} for _ in orders]
    last = None
    for position in range(len(offsets[0])):
        for segment in range(segments):
            o = offsets[segment][position]
            value, earlier = product(o, segment, held[last[0]][last[1]] if last else None)
            if last:
                held[last[0]][last[1]] = earlier
            held[segment][o] = value
            last = (segment, o)
    for stage in range(len(high_bits)):
        for segment, order in enumerate(orders):
            bit, sums = order[stage], held[segment]
            pairs = [(i, i ^ bit) for i in range(mp_size)]
            for o in sorted((o for o in sums if not o & bit), reverse=True):
                sums[o] = sums[o] + moved(sums.pop(o | bit), "mp", pairs)
    return [sums[0] for sums in held]


def summed(values, axes):
    for axis, size in axes:
        bit = 1
        while bit < size:
            values = values + lax.ppermute(values, axis, [(i, i ^ bit) for i in range(size)])
            bit *= 2
    return values


def local(mp_size, dp_size, crop_hidden, projector_weight, pairing):
    crop_count, local_rows, width_part = crop_hidden.shape
    features = projector_weight.shape[1]
    crops = crop_count // dp_size
    batch_rows = local_rows * dp_size
    me = lax.axis_index("dp")
    hidden = crop_hidden.reshape(dp_size, crops * local_rows, width_part)
    onehot = (pairing[:, :, None] == jnp.arange(local_rows, dtype=jnp.int32)[None, None, :]).astype(
        jnp.float32
    )
    invariance = 0.0
    owned = []
    for part in reduced_segments(hidden, projector_weight, mp_size):
        size = part.shape[1]
        pieces = [lax.dynamic_index_in_dim(part, me, axis=0, keepdims=False)]
        for shift in range(1, dp_size):
            pairs = [(i, (i + shift) % dp_size) for i in range(dp_size)]
            outgoing = lax.dynamic_index_in_dim(
                part, lax.rem(me + shift, dp_size), axis=0, keepdims=False
            )
            pieces.append(moved(outgoing, "dp", pairs))
        by_shift = jnp.stack(pieces[::-1], axis=0)
        by_source = jnp.roll(by_shift, me + 1, axis=0)
        owned.append(
            by_source.reshape(dp_size, size, crops, local_rows)
            .transpose(1, 2, 0, 3)
            .reshape(size, crops, batch_rows)
        )
        by_crop = part.reshape(dp_size, size, crops, local_rows).transpose(0, 2, 1, 3)
        by_crop = by_crop.reshape(crop_count, size, local_rows)
        aligned = jnp.einsum("cjr,cri->cji", by_crop, onehot, precision=lax.Precision.HIGH)
        for anchor in range(2):
            differ = aligned - aligned[anchor : anchor + 1]
            invariance = invariance + jnp.sum(differ * differ)
    owned_block = jnp.concatenate(owned, axis=0)
    column_mean = jnp.mean(owned_block, axis=2, keepdims=True)
    centered = owned_block - column_mean
    variance = jnp.sum(centered * centered, axis=2) / (batch_rows - 1)
    hinge_sum = jnp.sum(jax.nn.relu(1.0 - jnp.sqrt(variance + epsilon)))
    diagonal_sq = jnp.sum(variance * variance)
    gram_scale = 1.0 / ((batch_rows - 1) * (batch_rows - 1))
    narrow = centered.astype(jnp.bfloat16)
    partial_gram = jnp.einsum("jcr,jcs->crs", narrow, narrow, preferred_element_type=jnp.float32)
    partial_gram = partial_gram.reshape(crops * batch_rows, batch_rows).astype(jnp.bfloat16)
    gram_block = lax.psum_scatter(partial_gram, "mp", scatter_dimension=0, tiled=True).astype(
        jnp.float32
    )
    frobenius = jnp.sum(gram_block * gram_block) * gram_scale
    totals = summed(
        jnp.stack([invariance, hinge_sum, frobenius - diagonal_sq]),
        (("dp", dp_size), ("mp", mp_size)),
    )
    invariance_loss = totals[0] / (2 * (crop_count - 1) * batch_rows * features)
    variance_loss = totals[1] / (crop_count * features)
    covariance_loss = totals[2] / (crop_count * features)
    total_loss = 25.0 * invariance_loss + 25.0 * variance_loss + covariance_loss
    loss_terms = jnp.stack([invariance_loss, variance_loss, covariance_loss, total_loss])
    return (owned_block, loss_terms)


def solution(mesh):
    mp_size, dp_size = mesh.shape["mp"], mesh.shape["dp"]

    def step(crop_hidden, projector_weight, pairing):
        return local(mp_size, dp_size, crop_hidden, projector_weight, pairing)

    placed = (P(None, "dp", "mp"), P("mp", None), P(None, "dp"))
    return jax.shard_map(
        step, mesh=mesh, in_specs=placed, out_specs=(P("mp", "dp", None), P()), check_vma=False
    )
```

```python
import jax
import jax.numpy as jnp
from jax import lax
from jax.sharding import PartitionSpec as P

epsilon = 0.0001
groups = 2


def coded(values):
    top = jnp.maximum(jnp.max(jnp.abs(values), axis=-1, keepdims=True), 1e-30)
    codes = jnp.round(values * (32767.0 / top)).astype(jnp.int16)
    return codes, top * (1.0 / 32767.0)


def moved(values, axis, pairs):
    codes, step = coded(values)
    codes = lax.ppermute(codes, axis, pairs)
    step = lax.ppermute(step, axis, pairs)
    return codes.astype(jnp.float32) * step


def reduced_groups(hidden, weight, mp_size):
    me = lax.axis_index("mp")
    block = weight.shape[1] // mp_size
    size = block // groups
    partner = [(i, i ^ 1) for i in range(mp_size)]
    other_hidden = lax.ppermute(hidden, "mp", partner)
    high_bits = [1 << b for b in range(1, mp_size.bit_length() - 1)]

    def columns(relative, group, parity):
        start = (me ^ relative ^ parity) * block + group * size
        return lax.dynamic_slice_in_dim(weight, start, size, axis=1)

    def product(relative, group, earlier):
        mine = columns(relative, group, 0)
        theirs = lax.ppermute(columns(relative, group, 1), "mp", partner)
        if earlier is not None:
            mine, theirs, earlier = lax.optimization_barrier((mine, theirs, earlier))
        terms = [
            lax.dot_general(
                w, h, (((0,), (2,)), ((), ())), preferred_element_type=jnp.float32
            )
            for w, h in ((mine, hidden), (theirs, other_hidden))
        ]
        return (terms[0] + terms[1]).transpose(1, 0, 2), earlier

    listed = [0]
    for bit in high_bits[::-1]:
        listed = listed + [o | bit for o in listed]
    held = [{} for _ in range(groups)]
    last = None
    for group in range(groups):
        for o in listed[::-1]:
            value, earlier = product(o, group, held[last[0]][last[1]] if last else None)
            if last:
                held[last[0]][last[1]] = earlier
            held[group][o] = value
            last = (group, o)
    results = []
    for group in range(groups):
        halves = []
        for half, order in enumerate((high_bits, high_bits[::-1])):
            low = half * (size // 2)
            sums = {o: v[:, low : low + size // 2] for o, v in held[group].items()}
            for bit in order:
                pairs = [(i, i ^ bit) for i in range(mp_size)]
                for o in sorted((o for o in sums if not o & bit), reverse=True):
                    sums[o] = sums[o] + moved(sums.pop(o | bit), "mp", pairs)
            halves.append(sums[0])
        results.append(jnp.concatenate(halves, axis=1))
    return results


def summed(values, axes):
    for axis, size in axes:
        bit = 1
        while bit < size:
            values = values + lax.ppermute(values, axis, [(i, i ^ bit) for i in range(size)])
            bit *= 2
    return values


def local(mp_size, dp_size, crop_hidden, projector_weight, pairing):
    crop_count, local_rows, width_part = crop_hidden.shape
    features = projector_weight.shape[1]
    crops = crop_count // dp_size
    batch_rows = local_rows * dp_size
    me = lax.axis_index("dp")
    hidden = crop_hidden.reshape(dp_size, crops * local_rows, width_part)
    onehot = (pairing[:, :, None] == jnp.arange(local_rows, dtype=jnp.int32)[None, None, :]).astype(
        jnp.float32
    )
    invariance = 0.0
    owned = []
    for part in reduced_groups(hidden, projector_weight, mp_size):
        size = part.shape[1]
        pieces = [lax.dynamic_index_in_dim(part, me, axis=0, keepdims=False)]
        for shift in range(1, dp_size):
            pairs = [(i, (i + shift) % dp_size) for i in range(dp_size)]
            outgoing = lax.dynamic_index_in_dim(
                part, lax.rem(me + shift, dp_size), axis=0, keepdims=False
            )
            pieces.append(moved(outgoing, "dp", pairs))
        by_shift = jnp.stack(pieces[::-1], axis=0)
        by_source = jnp.roll(by_shift, me + 1, axis=0)
        owned.append(
            by_source.reshape(dp_size, size, crops, local_rows)
            .transpose(1, 2, 0, 3)
            .reshape(size, crops, batch_rows)
        )
        by_crop = part.reshape(dp_size, size, crops, local_rows).transpose(0, 2, 1, 3)
        by_crop = by_crop.reshape(crop_count, size, local_rows)
        aligned = jnp.einsum("cjr,cri->cji", by_crop, onehot, precision=lax.Precision.HIGH)
        for anchor in range(2):
            differ = aligned - aligned[anchor : anchor + 1]
            invariance = invariance + jnp.sum(differ * differ)
    owned_block = jnp.concatenate(owned, axis=0)
    column_mean = jnp.mean(owned_block, axis=2, keepdims=True)
    centered = owned_block - column_mean
    variance = jnp.sum(centered * centered, axis=2) / (batch_rows - 1)
    hinge_sum = jnp.sum(jax.nn.relu(1.0 - jnp.sqrt(variance + epsilon)))
    diagonal_sq = jnp.sum(variance * variance)
    gram_scale = 1.0 / ((batch_rows - 1) * (batch_rows - 1))
    narrow = centered.astype(jnp.bfloat16)
    partial_gram = jnp.einsum("jcr,jcs->crs", narrow, narrow, preferred_element_type=jnp.float32)
    partial_gram = partial_gram.reshape(crops * batch_rows, batch_rows).astype(jnp.bfloat16)
    gram_block = lax.psum_scatter(partial_gram, "mp", scatter_dimension=0, tiled=True).astype(
        jnp.float32
    )
    frobenius = jnp.sum(gram_block * gram_block) * gram_scale
    totals = summed(
        jnp.stack([invariance, hinge_sum, frobenius - diagonal_sq]),
        (("dp", dp_size), ("mp", mp_size)),
    )
    invariance_loss = totals[0] / (2 * (crop_count - 1) * batch_rows * features)
    variance_loss = totals[1] / (crop_count * features)
    covariance_loss = totals[2] / (crop_count * features)
    total_loss = 25.0 * invariance_loss + 25.0 * variance_loss + covariance_loss
    loss_terms = jnp.stack([invariance_loss, variance_loss, covariance_loss, total_loss])
    return (owned_block, loss_terms)


def solution(mesh):
    mp_size, dp_size = mesh.shape["mp"], mesh.shape["dp"]

    def step(crop_hidden, projector_weight, pairing):
        return local(mp_size, dp_size, crop_hidden, projector_weight, pairing)

    placed = (P(None, "dp", "mp"), P("mp", None), P(None, "dp"))
    return jax.shard_map(
        step, mesh=mesh, in_specs=placed, out_specs=(P("mp", "dp", None), P()), check_vma=False
    )
```
